32 devices in a mesh: groups: 2 (over y), seq: 4 (over z), fsdp: 2 (over x), sub: 2 (over core).
Axes of the slice: x: 2, y: 2, z: 4, core: 2. Of those that a mesh axis runs over, the one named last changes fastest.
Arguments:
- tokens: bfloat16 [2048, 8192], P(('groups', 'seq')), parts along dimension 0, may hold values from -400 to 400
- norm_gain: float32 [8192], replicated, may hold values from 0.1 to 1.9
- w_query: bfloat16 [8, 16, 8192], P(('seq', 'sub'), 'fsdp'), may hold values from -0.0625 to 0.0625
- w_key: bfloat16 [8, 16, 8192], P(('seq', 'sub'), 'fsdp'), may hold values from -0.0625 to 0.0625
- w_value: bfloat16 [8, 128, 8192], P(('seq', 'sub'), 'fsdp'), may hold values from -5 to 5
- head_gain: float32 [128], replicated, may hold values from 0.1 to 1.9
- w_out: bfloat16 [8, 128, 8192], P('seq', None, ('fsdp', 'sub')), may hold values from -0.1875 to 0.1875
Outputs:
- mixed: bfloat16 [2048, 8192], P(('groups', 'seq'), ('fsdp', 'sub')), parts along dimension 0
The draws below stay inside these ranges and needn't reach their ends.
There are 2 independent parts, one for each index of `groups`. The reference program is written for one: setup_inputs(seed, part) draws one part's arguments, and reference() takes and returns one part's arrays. A program takes and returns all parts, laid end to end along the dimension named above; an argument that names none is the same for every part. Nothing has to cross between parts.
All inputs are finite; a program needn't handle non-finite values.
Results may differ from the reference program's by a relative error of at most 0.0084.
Values may be sent and summed in bfloat16 or wider, within the bound.
No kernel may reach another device: no remote copies, remote signals or barrier semaphores. Data moves between devices by JAX's collectives and lax.ppermute only.
A program may use at most 64 MiB of HBM per device.

```python
import math
import jax
import jax.numpy as jnp
import numpy as np
from jax import lax

D = 8192
HEAD_DIM = 128
FEAT = 16
BLOCK = 512
HEADS = 8
L = 1024


def draw_tokens(key, part):
    subkeys = jax.random.split(jax.random.fold_in(key, 101), 3)
    row_scale = jnp.exp(jax.random.uniform(subkeys[0], (L, 1), jnp.float32, 0.0, math.log(10.0)))
    col_scale = jnp.exp(jax.random.uniform(subkeys[1], (1, D), jnp.float32, 0.0, math.log(10.0)))
    entries = jnp.clip(jax.random.normal(subkeys[2], (L, D), jnp.float32), -4.0, 4.0)
    return (entries * row_scale * col_scale).astype(jnp.bfloat16)


def draw_w_value(key, part):
    subkeys = jax.random.split(jax.random.fold_in(key, 202), 2)
    upward = jnp.arange(HEAD_DIM, dtype=jnp.float32)[None, :, None] / (HEAD_DIM - 1.0)
    jitter = jax.random.uniform(subkeys[0], (HEADS, HEAD_DIM, 1), jnp.float32, 0.0, 1.0)
    exponent = 0.5 * upward + 0.5 * jitter
    entries = jnp.clip(jax.random.normal(subkeys[1], (HEADS, HEAD_DIM, D), jnp.float32), -4.0, 4.0)
    factor = jnp.power(10.0, exponent) / math.sqrt(D)
    return (entries * factor).astype(jnp.bfloat16)


def levels(key, extent, cuts, low, top_value):
    gain, own = 1.0, jax.random.fold_in(key, 6)
    for position, parts in cuts:
        draws = jnp.exp(jax.random.uniform(jax.random.fold_in(own, position), (parts,), jnp.float32, low / len(cuts), top_value / len(cuts)))
        gain = gain * jnp.repeat(draws, extent[position] // parts).reshape([-1 if axis == position else 1 for axis in range(len(extent))])
    return gain


def centred(own_key, dims, width, limit, cuts=(), kind=jnp.bfloat16):
    drawn = jax.random.normal(own_key, dims, jnp.float32) * width
    if len(cuts) > 0:
        drawn = levels(own_key, dims, cuts, -0.22, 0.18) * drawn
    return jnp.clip(drawn, min=-limit, max=limit).astype(kind)


def setup_inputs(seed: int = 0, part: int = 0) -> dict:
    key_list = jax.random.split(jax.random.key(seed), 8)
    own_keys = jax.random.split(jax.random.fold_in(key_list[7], part), 8)
    tokens = draw_tokens(jax.random.fold_in(jax.random.fold_in(key_list[7], part), 71), part)
    norm_gain = jnp.clip(1.0 + 0.18 * jax.random.normal(key_list[1], (D,), jnp.float32), 0.1, 1.9)
    w_query = centred(key_list[2], (HEADS, FEAT, D), D ** -0.5, 0.0625, ((0, 8), (1, 2)))
    w_key = centred(key_list[3], (HEADS, FEAT, D), D ** -0.5, 0.0625, ((0, 8), (1, 2)))
    w_value = draw_w_value(jax.random.fold_in(key_list[7], 71), part)
    head_gain = jnp.clip(1.0 + 0.18 * jax.random.normal(key_list[5], (HEAD_DIM,), jnp.float32), 0.1, 1.9)
    w_out = centred(key_list[6], (HEADS, HEAD_DIM, D), (HEADS * HEAD_DIM) ** -0.5, 0.1875, ((0, 4), (2, 4)))
    return dict(tokens=tokens, norm_gain=norm_gain, w_query=w_query, w_key=w_key, w_value=w_value, head_gain=head_gain, w_out=w_out)


def taylor_last(vectors):
    feature_count = vectors.shape[-1]
    first_row, second_row = np.triu_indices(feature_count, 1)
    cross_terms = vectors[..., first_row] * vectors[..., second_row] / 4.0
    squares = vectors * vectors / (4.0 * math.sqrt(2.0))
    leading = jnp.ones(vectors.shape[:-1] + (1,), jnp.float32)
    return jnp.concatenate([leading, vectors / 2.0, cross_terms, squares], -1)

def reference(tokens, norm_gain, w_query, w_key, w_value, head_gain, w_out):
    inputs = tokens.astype(jnp.float32)
    meansq = lax.optimization_barrier(jnp.mean(inputs * inputs, axis=-1, keepdims=True))
    normed = (inputs * lax.rsqrt(meansq + 1e-05) * norm_gain).astype(jnp.bfloat16)
    length = tokens.shape[0]

    def project(weight):
        flattened = weight.reshape(-1, weight.shape[-1])
        result = jnp.dot(normed, flattened.T, preferred_element_type=jnp.float32)
        result = result.astype(jnp.bfloat16).reshape(length, weight.shape[0], weight.shape[1])
        return jnp.transpose(result, (1, 0, 2))
    queries = project(w_query)
    key_vectors = project(w_key)
    values_all = project(w_value)
    nblocks = length // BLOCK
    position_t = jnp.arange(BLOCK, dtype=jnp.int32)[:, None]
    position_j = jnp.arange(BLOCK, dtype=jnp.int32)[None, :]
    causal = position_j <= position_t

    def one_head(operands):
        head_query, head_key, head_value = operands
        query_feats = taylor_last(head_query.astype(jnp.float32)).astype(jnp.bfloat16)
        key_feats = taylor_last(head_key.astype(jnp.float32)).astype(jnp.bfloat16)
        key_blocks = key_feats.astype(jnp.float32).reshape(nblocks, BLOCK, -1)
        value_blocks = head_value.astype(jnp.float32).reshape(nblocks, BLOCK, -1)
        contrib = jnp.einsum('bjf,bje->bfe', key_blocks, value_blocks)
        prefix = jnp.concatenate([jnp.zeros_like(contrib[:1]), jnp.cumsum(contrib[:-1], axis=0)], 0)
        prior_state = prefix.astype(jnp.bfloat16)
        query_blocks = head_query.astype(jnp.float32).reshape(nblocks, BLOCK, -1)
        raw_keys = head_key.astype(jnp.float32).reshape(nblocks, BLOCK, -1)
        scores = jnp.einsum('btf,bjf->btj', query_blocks, raw_keys)
        kernel = 1.0 + scores / 4.0 + scores * scores / 32.0
        weight = jnp.where(causal[None], kernel, 0.0).astype(jnp.bfloat16)
        local_part = jnp.einsum('btj,bje->bte', weight.astype(jnp.float32), value_blocks)
        feat_blocks = query_feats.astype(jnp.float32).reshape(nblocks, BLOCK, -1)
        carried = jnp.einsum('btf,bfe->bte', feat_blocks, prior_state.astype(jnp.float32))
        return (local_part + carried).reshape(length, -1).astype(jnp.bfloat16)
    numerator = lax.map(one_head, (queries, key_vectors, values_all))
    widened = numerator.astype(jnp.float32)
    meansq_out = lax.optimization_barrier(jnp.mean(widened * widened, axis=-1, keepdims=True))
    attended = (widened * lax.rsqrt(meansq_out + 1e-06) * head_gain).astype(jnp.bfloat16)
    flat_att = jnp.transpose(attended, (1, 0, 2)).reshape(length, -1)
    out_rows = w_out.reshape(-1, w_out.shape[-1])
    return jnp.dot(flat_att, out_rows, preferred_element_type=jnp.float32).astype(jnp.bfloat16)
```

```python
import jax
import jax.numpy as jnp
from jax import lax
from jax.sharding import PartitionSpec as P

QUERY_CHUNK = 512


def head_norm(numerator, head_gain, channel_axis):
    widened = numerator.astype(jnp.float32)
    meansq = jnp.mean(widened * widened, axis=channel_axis, keepdims=True)
    gain_shape = tuple((-1 if axis_pos == channel_axis else 1 for axis_pos in range(widened.ndim)))
    return (widened * lax.rsqrt(meansq + 1e-06) * head_gain.reshape(gain_shape)).astype(
        jnp.bfloat16
    )


def absolute_order(pieces, group):
    count = len(pieces)
    ordered = []
    for target in range(count):
        chosen = pieces[0]
        for offset in range(1, count):
            chosen = jnp.where((group - offset) % count == target, pieces[offset], chosen)
        ordered.append(chosen)
    return ordered


def spread(own):
    groups, seq = lax.axis_size("groups"), lax.axis_size("seq")
    here = lax.axis_index("seq")
    up, down = [own], [own]
    for _ in range(1, seq):
        up.append(lax.ppermute(up[-1], "seq", [(i, i + 1) for i in range(seq - 1)]))
        down.append(lax.ppermute(down[-1], "seq", [(i + 1, i) for i in range(seq - 1)]))

    def across(array, hops, upward, offset):
        if offset == 0:
            return array
        places = range(hops, seq) if upward else range(seq - hops)
        pairs = [
            (g * seq + i, ((g + offset) % groups) * seq + i) for g in range(groups) for i in places
        ]
        return lax.ppermute(array, ("groups", "seq"), pairs)

    slots = []
    for k in range(1, seq):
        pieces = []
        for offset in range(groups):
            from_below = across(up[k], k, True, offset)
            from_above = across(down[seq - k], seq - k, False, offset)
            pieces.append((from_below, from_above, here >= k))
        slots.append(pieces)
    return slots


def per_device(tokens, norm_gain, w_query, w_key, w_value, head_gain, w_out):
    groups, seq = lax.axis_size("groups"), lax.axis_size("seq")
    group, here = lax.axis_index("groups"), lax.axis_index("seq")
    feat_dev = w_query.shape[1]
    rows_here = tokens.shape[0]

    stacked = jnp.concatenate([w_query[0], w_key[0], w_value[0]], 0)
    part = stacked.shape[0] // groups
    w_slots = spread(lax.dynamic_slice_in_dim(stacked, group * part, part, 0))
    cols = w_out.shape[2] // groups
    own_cols = lax.dynamic_slice_in_dim(w_out, group * cols, cols, 2)

    inputs = tokens.astype(jnp.float32)
    meansq = jnp.mean(inputs * inputs, axis=1, keepdims=True)
    normed = (inputs * lax.rsqrt(meansq + 1e-05) * norm_gain).astype(jnp.bfloat16)
    normed = lax.optimization_barrier(normed)

    def project(weight):
        return jnp.einsum(
            "cd,td->ct", weight, normed, preferred_element_type=jnp.float32
        ).astype(jnp.bfloat16)

    arrived = [project(stacked)]
    for k in range(1, seq):
        pieces = [project(jnp.where(ok, below, above)) for below, above, ok in w_slots[k - 1]]
        whole = jnp.concatenate(absolute_order(pieces, group), 0)
        arrived.append(lax.ppermute(whole, "seq", [(i, (i - k) % seq) for i in range(seq)]))
    by_head = jnp.concatenate(arrived, 1)
    length = by_head.shape[1]
    qk_whole = lax.all_gather(by_head[: 2 * feat_dev], "fsdp", axis=0)
    values_local = by_head[2 * feat_dev :]
    queries = qk_whole[:, :feat_dev].reshape(-1, length)
    key_vectors = qk_whole[:, feat_dev:].reshape(-1, length)

    def positions(shape, axis, start):
        index = lax.broadcasted_iota(jnp.int32, shape, axis) + start
        return (index + here * rows_here) % length

    numerators = []
    chunk = min(QUERY_CHUNK, length)
    for start in range(0, length, chunk):
        scores = jnp.einsum(
            "fj,ft->jt",
            key_vectors,
            queries[:, start : start + chunk],
            preferred_element_type=jnp.float32,
        )
        kernel = 1.0 + scores / 4.0 + scores * scores / 32.0
        causal = positions((length, 1), 0, 0) <= positions((1, chunk), 1, start)
        weight = jnp.where(causal, kernel, 0.0).astype(jnp.bfloat16)
        numerators.append(
            jnp.einsum("ej,jt->et", values_local, weight, preferred_element_type=jnp.float32)
        )
    numerator = jnp.concatenate(numerators, 1).astype(jnp.bfloat16)

    w_out_slots = spread(own_cols)
    returned = []
    for k in range(seq):
        piece = numerator[:, k * rows_here : (k + 1) * rows_here]
        if k:
            piece = lax.ppermute(piece, "seq", [(i, (i + k) % seq) for i in range(seq)])
        returned.append(piece)
    by_token = jnp.stack(returned)
    everyone = lax.all_gather(by_token, ("fsdp", "sub"), axis=0)
    arranged = everyone.reshape((lax.axis_size("fsdp"), lax.axis_size("sub")) + by_token.shape)
    arranged = jnp.transpose(arranged, (2, 1, 0, 3, 4))
    arranged = arranged.reshape(-1, w_out.shape[1], rows_here)
    attended = head_norm(arranged, head_gain, 1)
    outputs = []
    for offset in range(groups):
        first = lax.dynamic_slice_in_dim(w_out, ((group - offset) % groups) * cols, cols, 2)
        blocks = [first]
        for k in range(1, seq):
            below, above, ok = w_out_slots[k - 1][offset]
            blocks.append(jnp.where(ok, below, above))
        outputs.append(
            jnp.einsum(
                "het,hed->td",
                attended,
                jnp.concatenate(blocks, 0),
                preferred_element_type=jnp.float32,
            ).astype(jnp.bfloat16)
        )
    return jnp.concatenate(absolute_order(outputs, group), 1)


def solution(mesh):
    in_specs = (
        P(("groups", "seq"), None),
        P(),
        P(("seq", "sub"), "fsdp", None),
        P(("seq", "sub"), "fsdp", None),
        P(("seq", "sub"), "fsdp", None),
        P(),
        P("seq", None, ("fsdp", "sub")),
    )
    out_specs = P(("groups", "seq"), ("fsdp", "sub"))
    return jax.shard_map(
        per_device, mesh=mesh, in_specs=in_specs, out_specs=out_specs, check_vma=False
    )
```

```python
import math

import jax
import jax.numpy as jnp
from jax import lax
from jax.sharding import PartitionSpec as P

QUERY_CHUNK = 512


def head_norm(numerator, head_gain, channel_axis):
    widened = numerator.astype(jnp.float32)
    meansq = jnp.mean(widened * widened, axis=channel_axis, keepdims=True)
    gain_shape = tuple((-1 if axis_pos == channel_axis else 1 for axis_pos in range(widened.ndim)))
    return (widened * lax.rsqrt(meansq + 1e-06) * head_gain.reshape(gain_shape)).astype(
        jnp.bfloat16
    )


def exchange(array, axes, distance):
    sizes = [lax.axis_size(axis) for axis in axes]
    total = math.prod(sizes)
    pairs = []
    for flat in range(total):
        target, scale, rest = 0, 1, flat
        for size, step in zip(reversed(sizes), reversed(distance)):
            target += ((rest % size) ^ step) * scale
            rest //= size
            scale *= size
        pairs.append((flat, target))
    return lax.ppermute(array, tuple(axes), pairs)


def spread(own, axis):
    size = lax.axis_size(axis)
    slots = [own] + [None] * (size - 1)
    bit = size // 2
    while bit:
        for k in range(0, size, 2 * bit):
            slots[k + bit] = exchange(slots[k], (axis,), (bit,))
        bit //= 2
    return slots


def absolute_order(slots, here):
    ordered = []
    for target in range(len(slots)):
        chosen = slots[target]
        for k in range(1, len(slots)):
            chosen = jnp.where(here == k, slots[target ^ k], chosen)
        ordered.append(chosen)
    return ordered


def per_device(tokens, norm_gain, w_query, w_key, w_value, head_gain, w_out):
    groups, seq = lax.axis_size("groups"), lax.axis_size("seq")
    group, here = lax.axis_index("groups"), lax.axis_index("seq")
    feat_dev = w_query.shape[1]
    rows_here = tokens.shape[0]

    stacked = jnp.concatenate([w_query[0], w_key[0], w_value[0]], 0)
    part = stacked.shape[0] // groups
    own_rows = lax.dynamic_slice_in_dim(stacked, group * part, part, 0)
    w_slots = spread(own_rows, "seq")
    cols = w_out.shape[2] // groups
    own_cols = lax.dynamic_slice_in_dim(w_out, group * cols, cols, 2)
    own_cols, w_slots[seq // 2] = lax.optimization_barrier((own_cols, w_slots[seq // 2]))
    w_out_slots = spread(own_cols, "seq")

    inputs = tokens.astype(jnp.float32)
    meansq = jnp.mean(inputs * inputs, axis=1, keepdims=True)
    normed = (inputs * lax.rsqrt(meansq + 1e-05) * norm_gain).astype(jnp.bfloat16)
    normed = lax.optimization_barrier(normed)

    def project(weight):
        return jnp.einsum(
            "cd,td->ct", weight, normed, preferred_element_type=jnp.float32
        ).astype(jnp.bfloat16)

    fsdp = lax.axis_size("fsdp")
    arrived, qk_arrived = [], [[] for _ in range(fsdp)]
    for k in range(seq):
        if k:
            pieces = [
                project(w_slots[k] if not o else exchange(w_slots[k], ("groups",), (o,)))
                for o in range(groups)
            ]
            whole = jnp.concatenate(absolute_order(pieces, group), 0)
        else:
            whole = project(stacked)
        for m in range(1, fsdp):
            qk_arrived[m].append(exchange(whole[: 2 * feat_dev], ("seq", "fsdp"), (k, m)))
        whole = exchange(whole, ("seq",), (k,)) if k else whole
        qk_arrived[0].append(whole[: 2 * feat_dev])
        arrived.append(whole[2 * feat_dev :])
    values_local = jnp.concatenate(arrived, 1)
    length = values_local.shape[1]
    queries = jnp.concatenate(
        [jnp.concatenate([piece[:feat_dev] for piece in row], 1) for row in qk_arrived], 0
    )
    key_vectors = jnp.concatenate(
        [jnp.concatenate([piece[feat_dev:] for piece in row], 1) for row in qk_arrived], 0
    )

    def positions(shape, axis, start):
        index = lax.broadcasted_iota(jnp.int32, shape, axis) + start
        return ((index // rows_here) ^ here) * rows_here + index % rows_here

    numerators = []
    chunk = min(QUERY_CHUNK, length)
    for start in range(0, length, chunk):
        scores = jnp.einsum(
            "fj,ft->jt",
            key_vectors,
            queries[:, start : start + chunk],
            preferred_element_type=jnp.float32,
        )
        kernel = 1.0 + scores / 4.0 + scores * scores / 32.0
        causal = positions((length, 1), 0, 0) <= positions((1, chunk), 1, start)
        weight = jnp.where(causal, kernel, 0.0).astype(jnp.bfloat16)
        numerators.append(
            jnp.einsum("ej,jt->et", values_local, weight, preferred_element_type=jnp.float32)
        )
    numerator = jnp.concatenate(numerators, 1).astype(jnp.bfloat16)

    returned = []
    for k in range(seq):
        piece = numerator[:, k * rows_here : (k + 1) * rows_here]
        returned.append(exchange(piece, ("seq",), (k,)) if k else piece)
    by_token = jnp.stack(returned)
    both = absolute_order(spread(by_token, "fsdp"), lax.axis_index("fsdp"))
    whole_heads = jnp.concatenate(both, 1)
    heads = absolute_order(spread(whole_heads, "sub"), lax.axis_index("sub"))
    arranged = jnp.stack(heads, 1).reshape(-1, w_out.shape[1], rows_here)
    attended = head_norm(arranged, head_gain, 1)
    outputs = []
    for o in range(groups):
        blocks = [lax.dynamic_slice_in_dim(w_out, (group ^ o) * cols, cols, 2)]
        for k in range(1, seq):
            slot = w_out_slots[k]
            blocks.append(exchange(slot, ("groups",), (o,)) if o else slot)
        outputs.append(
            jnp.einsum(
                "het,hed->td",
                attended,
                jnp.concatenate(blocks, 0),
                preferred_element_type=jnp.float32,
            ).astype(jnp.bfloat16)
        )
    return jnp.concatenate(absolute_order(outputs, group), 1)


def solution(mesh):
    in_specs = (
        P(("groups", "seq"), None),
        P(),
        P(("seq", "sub"), "fsdp", None),
        P(("seq", "sub"), "fsdp", None),
        P(("seq", "sub"), "fsdp", None),
        P(),
        P("seq", None, ("fsdp", "sub")),
    )
    out_specs = P(("groups", "seq"), ("fsdp", "sub"))
    return jax.shard_map(
        per_device, mesh=mesh, in_specs=in_specs, out_specs=out_specs, check_vma=False
    )
```
